32 devices in a mesh: batch: 1 (over z), cy: 4 (over y), cx: 8 (over x, core).
Axes of the slice: x: 4, y: 4, z: 1, core: 2. Of those that a mesh axis runs over, the one named last changes fastest.
The devices are a block of a 4x4x8 slice.
Arguments:
- q_seq: bfloat16 [8192, 14, 64], P(('batch', 'cx', 'cy'))
- k_seq: bfloat16 [8192, 2, 64], P(('batch', 'cx', 'cy'))
- v_seq: bfloat16 [8192, 2, 64], P(('batch', 'cx', 'cy'))
Outputs:
- output: bfloat16 [8192, 14, 64], P(('batch', 'cx', 'cy'))
All inputs are finite; a program needn't handle non-finite values.
Results may differ from the reference program's by a relative error of at most 0.00489606.
Values are sent between devices in bfloat16 or wider.
A program may use at most 768 MiB of HBM per device.

```python
import math
import jax
import jax.numpy as jnp
from jax import lax

SEQ = 8192
HEADS = 14
KV_HEADS = 2
HEAD = 64
Q_BLOCK = 32

GROUP_HEADS = HEADS // KV_HEADS
SCORE_STD = math.sqrt(max(1.0, math.log(SEQ / 64.0)))


def setup_inputs(seed: int = 0, part: int = 0) -> dict:
    base_key = jax.random.fold_in(jax.random.key(seed), part)
    key_q, key_k, key_v = jax.random.split(base_key, 3)
    in_scale = math.sqrt(SCORE_STD)
    q_seq = jax.random.normal(key_q, (SEQ, HEADS, HEAD), jnp.float32) * in_scale
    k_seq = jax.random.normal(key_k, (SEQ, KV_HEADS, HEAD), jnp.float32) * in_scale
    v_seq = jax.random.normal(key_v, (SEQ, KV_HEADS, HEAD), jnp.float32) * 2.0
    return {"q_seq": q_seq.astype(jnp.bfloat16), "k_seq": k_seq.astype(jnp.bfloat16), "v_seq": v_seq.astype(jnp.bfloat16)}


def reference(q_seq, k_seq, v_seq):
    score_scale = 1.0 / math.sqrt(HEAD)
    keys_wide = k_seq.astype(jnp.float32)
    vals_wide = v_seq.astype(jnp.float32)
    q_blocks = q_seq.reshape(SEQ // Q_BLOCK, Q_BLOCK, KV_HEADS, GROUP_HEADS, HEAD)

    def attend_block(q_part):
        scores = jnp.einsum("qkgd,skd->kgqs", q_part.astype(jnp.float32), keys_wide) * score_scale
        row_max = jnp.max(scores, axis=-1, keepdims=True)
        prob_all = jnp.exp(scores - row_max)
        row_sum = jnp.sum(prob_all, axis=-1)
        weighted = jnp.einsum("kgqs,skd->qkgd", prob_all.astype(jnp.bfloat16).astype(jnp.float32), vals_wide)
        result = weighted / jnp.transpose(row_sum, (2, 0, 1))[..., None]
        return result.astype(jnp.bfloat16)

    out_blocks = lax.map(attend_block, q_blocks)
    return out_blocks.reshape(SEQ, HEADS, HEAD)
```

```python
import functools
import math
import jax
import jax.numpy as jnp
from jax import lax
from jax.experimental import pallas as pl
from jax.experimental.pallas import tpu as pltpu
from jax.sharding import PartitionSpec as P

SLOTS = [(0, 0), (1, 0), (-1, 0), (0, 1), (0, -1), (1, 1), (1, -1), (-1, 1), (-1, -1), (2, 0), (0, 2),
         (2, 1), (2, -1), (1, 2), (-1, 2), (2, 2)]
SLOT_OF = {offset: slot for slot, offset in enumerate(SLOTS)}
LAG = 2


def wrap(step):
    return (step + 1) % 4 - 1


def send_plan():
    plan = {}

    def add(what, offset, step_x, step_y):
        plan.setdefault((what, SLOT_OF[offset]), []).append((step_x, step_y))

    for what, swap in (("k", False), ("v", True)):
        flip = (lambda pair: (pair[1], pair[0])) if swap else (lambda pair: pair)
        sign = -1 if swap else 1

        def hop(offset, step):
            add(what, flip(offset), *flip(step))

        hop((0, 0), (1, 0))
        hop((0, 0), (-1, 0))
        hop((-sign, 0), (sign, 0))
        for dx in (0, 1, -1, 2):
            hop((dx, 0), (0, 1))
            hop((dx, 0), (0, -1))
            way = sign if dx in (0, 1) else -sign
            hop((dx, -way), (0, way))
    return plan


PLAN = send_plan()
RELAY = {1: (1, 2, 3, 4), 5: (5, 6, 7, 8, 9, 10), 8: (11, 12, 13, 14), 13: (15,)}


def split3(wide):
    hi = wide.astype(jnp.bfloat16)
    rest = wide - hi.astype(jnp.float32)
    mid = rest.astype(jnp.bfloat16)
    low = (rest - mid.astype(jnp.float32)).astype(jnp.bfloat16)
    return hi, mid, low


def attention_kernel(size_x, size_y, q_ref, k_ref, v_ref, o_ref, kbuf, vbuf, qw, kk, m_s, l_s, acc, sbuf,
                     send_sem, recv_k, recv_v):
    heads, head_dim, tokens = q_ref.shape
    num_kv = k_ref.shape[0] // head_dim
    group = heads // num_kv
    slots = len(SLOTS)
    cx, cy = lax.axis_index("cx"), lax.axis_index("cy")
    core = cx % 2
    chip_x = cx // 2

    def peer(step_x, step_y):
        return {"cx": ((chip_x + step_x + size_x) % size_x) * 2 + core, "cy": (cy + step_y + size_y) % size_y}

    sibling = {"cx": chip_x * 2 + (1 - core), "cy": cy}
    mesh_id = pl.DeviceIdType.MESH

    barrier = pltpu.get_barrier_semaphore()
    for device in (peer(1, 0), peer(-1, 0), peer(0, 1), peer(0, -1), sibling):
        pl.semaphore_signal(barrier, inc=1, device_id=device, device_id_type=mesh_id)
    pl.semaphore_wait(barrier, 5)

    bufs = {"k": (kbuf, recv_k, k_ref), "v": (vbuf, recv_v, v_ref)}
    copies = []

    def here(what, slot):
        buf, _, own = bufs[what]
        return own if slot == 0 else buf.at[slot, 0]

    def push(what, slot, dst_slot, plane, device):
        buf, recv, _ = bufs[what]
        copies.append((what, slot))
        pltpu.make_async_remote_copy(
            src_ref=here(what, slot), dst_ref=buf.at[dst_slot, plane], send_sem=send_sem.at[len(copies) - 1],
            recv_sem=recv.at[dst_slot, plane], device_id=device, device_id_type=mesh_id).start()

    def pass_on(what, slot):
        for step_x, step_y in PLAN.get((what, slot), ()):
            dx, dy = SLOTS[slot]
            push(what, slot, SLOT_OF[(wrap(dx - step_x), wrap(dy - step_y))], 0, peer(step_x, step_y))
        push(what, slot, slot, 1, sibling)

    def arrived(what, slot, plane):
        buf, recv, _ = bufs[what]
        pltpu.make_async_copy(buf.at[slot, plane], buf.at[slot, plane], recv.at[slot, plane]).wait()

    pass_on("k", 0)
    pass_on("v", 0)

    scale = math.log2(math.e) / math.sqrt(head_dim)
    for h in range(heads):
        hi, mid, low = split3(q_ref[h].astype(jnp.float32) * scale)
        qw[h, 0:head_dim] = hi
        qw[h, head_dim:2 * head_dim] = mid
        qw[h, 2 * head_dim:3 * head_dim] = low
        qw[h, 3 * head_dim:] = jnp.zeros_like(hi)
    m_s[...] = jnp.full(m_s.shape, -jnp.inf, jnp.float32)
    for ref in (l_s, acc):
        ref[...] = jnp.zeros(ref.shape, ref.dtype)
    vbuf[0, 0] = v_ref[...]

    def lay_out(slot, plane):
        own = slot == 0 and plane == 0
        for g in range(num_kv):
            part = slice(g * head_dim, (g + 1) * head_dim)
            kt = k_ref[part] if own else kbuf[slot, plane, part]
            kk[slot, g, plane] = jnp.concatenate([kt, kt], axis=0).T

    def make_ready(slot):
        for relay in RELAY.get(slot, ()):
            for what in ("k", "v"):
                arrived(what, relay, 0)
                pass_on(what, relay)
        for what in ("k", "v"):
            arrived(what, slot, 1)
        for plane in range(2):
            lay_out(slot, plane)

    def step(i, carry):
        for s in range(1, slots):
            @pl.when(i == s)
            def _():
                make_ready(s)
        tops = {}

        def scores(h, m):
            keys = kk[i, h // group, m]
            s = jnp.dot(jnp.concatenate([keys, keys], axis=1), qw[h], preferred_element_type=jnp.float32)
            sbuf[h % (LAG + 1), m * tokens:(m + 1) * tokens] = s
            top = jnp.max(s.reshape(tokens // 8, 8, tokens), axis=0)
            tops[h] = top if m == 0 else jnp.maximum(tops[h], top)

        for h in range(LAG):
            for m in range(2):
                scores(h, m)
        for h in range(heads):
            g = h // group
            m_prev = m_s[h]
            m_new = jnp.maximum(m_prev, jnp.max(tops[h], axis=0, keepdims=True))
            m_s[h] = m_new
            alpha = jnp.exp2(m_prev - m_new)
            total = l_s[h] * alpha
            out = (acc[h].reshape(head_dim // 8, 8, tokens) * alpha[None]).reshape(head_dim, tokens)
            for m in range(2):
                if h + LAG < heads:
                    scores(h + LAG, m)
                p = jnp.exp2(sbuf[h % (LAG + 1), m * tokens:(m + 1) * tokens].reshape(tokens // 8, 8, tokens) - m_new[None])
                total = total + jnp.sum(p, axis=0)
                out = out + jnp.dot(vbuf[i, m, g * head_dim:(g + 1) * head_dim],
                                    p.reshape(tokens, tokens).astype(jnp.bfloat16), preferred_element_type=jnp.float32)
            l_s[h] = total
            acc[h] = out
        return carry

    make_ready(0)
    lax.fori_loop(0, slots, step, 0)
    for h in range(heads):
        total = jnp.sum(l_s[h], axis=0, keepdims=True)
        o_ref[h] = (acc[h] / total).astype(jnp.bfloat16)
    for n, (what, slot) in enumerate(copies):
        pltpu.make_async_copy(here(what, slot), here(what, slot), send_sem.at[n]).wait()


def solution(mesh):
    size_x = mesh.shape["cx"] // 2
    size_y = mesh.shape["cy"]
    seq_spec = P(("batch", "cx", "cy"), None, None)

    def local_attention(q_local, k_local, v_local):
        tokens, heads, head_dim = q_local.shape
        num_kv = k_local.shape[1]
        q_t = jnp.transpose(q_local, (1, 2, 0))
        k_t = jnp.transpose(k_local, (1, 2, 0)).reshape(num_kv * head_dim, tokens)
        v_t = jnp.transpose(v_local, (1, 2, 0)).reshape(num_kv * head_dim, tokens)
        slots = len(SLOTS)
        f32, bf16 = jnp.float32, jnp.bfloat16
        out = pl.pallas_call(
            functools.partial(attention_kernel, size_x, size_y),
            out_shape=jax.ShapeDtypeStruct((heads, head_dim, tokens), bf16),
            in_specs=[pl.BlockSpec(memory_space=pltpu.VMEM)] * 3,
            out_specs=pl.BlockSpec(memory_space=pltpu.VMEM),
            scratch_shapes=[
                pltpu.VMEM((slots, 2, num_kv * head_dim, tokens), bf16),
                pltpu.VMEM((slots, 2, num_kv * head_dim, tokens), bf16),
                pltpu.VMEM((heads, 256, tokens), bf16),
                pltpu.VMEM((slots, num_kv, 2, tokens, 2 * head_dim), bf16),
                pltpu.VMEM((heads, 8, tokens), f32),
                pltpu.VMEM((heads, 8, tokens), f32),
                pltpu.VMEM((heads, head_dim, tokens), f32),
                pltpu.VMEM((LAG + 1, 2 * tokens, tokens), f32),
                pltpu.SemaphoreType.DMA((64,)),
                pltpu.SemaphoreType.DMA((slots, 2)),
                pltpu.SemaphoreType.DMA((slots, 2)),
            ],
            compiler_params=pltpu.CompilerParams(
                collective_id=0, has_side_effects=True, vmem_limit_bytes=48 * 2**20),
            name="attention",
        )(q_t, k_t, v_t)
        return jnp.transpose(out, (2, 0, 1))

    return jax.shard_map(local_attention, mesh=mesh, in_specs=(seq_spec, seq_spec, seq_spec), out_specs=seq_spec, check_vma=False)
```

```python
import functools
import math
import jax
import jax.numpy as jnp
from jax import lax
from jax.experimental import pallas as pl
from jax.experimental.pallas import tpu as pltpu
from jax.sharding import PartitionSpec as P

SLOTS = [(0, 0), (1, 0), (-1, 0), (0, 1), (0, -1), (1, 1), (1, -1), (-1, 1), (-1, -1), (2, 0), (0, 2),
         (2, 1), (2, -1), (1, 2), (-1, 2), (2, 2)]
SLOT_OF = {offset: slot for slot, offset in enumerate(SLOTS)}
LAG = 3
VALUE_LAG = 2
CHUNK = 64
DEPTH = 4


def wrap(step):
    return (step + 1) % 4 - 1


def send_plan():
    plan = {}

    def add(what, offset, step_x, step_y):
        plan.setdefault((what, SLOT_OF[offset]), []).append((step_x, step_y))

    for what, swap in (("k", False), ("v", True)):
        flip = (lambda pair: (pair[1], pair[0])) if swap else (lambda pair: pair)
        sign = -1 if swap else 1

        def hop(offset, step):
            add(what, flip(offset), *flip(step))

        hop((0, 0), (1, 0))
        hop((0, 0), (-1, 0))
        hop((-sign, 0), (sign, 0))
        for dx in (0, 1, -1, 2):
            hop((dx, 0), (0, 1))
            hop((dx, 0), (0, -1))
            way = sign if dx in (0, 1) else -sign
            hop((dx, -way), (0, way))
    return plan


PLAN = send_plan()
RELAY = {1: (1, 2, 3, 4), 5: (5, 6, 7, 8, 9, 10), 8: (11, 12, 13, 14), 13: (15,)}


def split3(wide):
    hi = wide.astype(jnp.bfloat16)
    rest = wide - hi.astype(jnp.float32)
    mid = rest.astype(jnp.bfloat16)
    low = (rest - mid.astype(jnp.float32)).astype(jnp.bfloat16)
    return hi, mid, low


def attention_kernel(size_x, size_y, q_hbm, k_hbm, v_hbm, o_ref, q_ref, kbuf, vbuf, qw, kk, m_s, l_s, acc, load_sem,
                     send_sem, recv_k, recv_v, *rings):
    heads, head_dim, tokens = q_ref.shape
    num_kv = kbuf.shape[2] // head_dim
    group = heads // num_kv
    slots = len(SLOTS)
    s_ring, p_ring = rings[:LAG + 1], rings[LAG + 1:]
    cx, cy = lax.axis_index("cx"), lax.axis_index("cy")
    core = cx % 2
    chip_x = cx // 2

    def peer(step_x, step_y):
        return {"cx": ((chip_x + step_x + size_x) % size_x) * 2 + core, "cy": (cy + step_y + size_y) % size_y}

    sibling = {"cx": chip_x * 2 + (1 - core), "cy": cy}
    mesh_id = pl.DeviceIdType.MESH

    loads = [pltpu.make_async_copy(src, dst, load_sem.at[n]) for n, (src, dst) in enumerate(
        ((k_hbm, kbuf.at[0, 0]), (v_hbm, vbuf.at[0, 0]), (q_hbm, q_ref)))]
    for load in loads:
        load.start()
    barrier = pltpu.get_barrier_semaphore()
    for device in (peer(1, 0), peer(-1, 0), peer(0, 1), peer(0, -1), sibling):
        pl.semaphore_signal(barrier, inc=1, device_id=device, device_id_type=mesh_id)
    pl.semaphore_wait(barrier, 5)

    bufs = {"k": (kbuf, recv_k), "v": (vbuf, recv_v)}
    copies = []

    def push(what, slot, dst_slot, plane, device):
        buf, recv = bufs[what]
        copies.append((what, slot))
        pltpu.make_async_remote_copy(
            src_ref=buf.at[slot, 0], dst_ref=buf.at[dst_slot, plane], send_sem=send_sem.at[len(copies) - 1],
            recv_sem=recv.at[dst_slot, plane], device_id=device, device_id_type=mesh_id).start()

    def pass_on(what, slot):
        for step_x, step_y in PLAN.get((what, slot), ()):
            dx, dy = SLOTS[slot]
            push(what, slot, SLOT_OF[(wrap(dx - step_x), wrap(dy - step_y))], 0, peer(step_x, step_y))
        push(what, slot, slot, 1, sibling)

    def arrived(what, slot, plane):
        buf, recv = bufs[what]
        pltpu.make_async_copy(buf.at[slot, plane], buf.at[slot, plane], recv.at[slot, plane]).wait()

    for what, load in zip(("k", "v"), loads):
        load.wait()
        pass_on(what, 0)
    loads[2].wait()

    scale = math.log2(math.e) / math.sqrt(head_dim)
    for h in range(heads):
        hi, mid, low = split3(q_ref[h].astype(jnp.float32) * scale)
        qw[h, 0:head_dim] = hi
        qw[h, head_dim:2 * head_dim] = mid
        qw[h, 2 * head_dim:3 * head_dim] = low
        qw[h, 3 * head_dim:] = jnp.zeros_like(hi)
    m_s[...] = jnp.full(m_s.shape, -jnp.inf, jnp.float32)
    for ref in (l_s, acc):
        ref[...] = jnp.zeros(ref.shape, ref.dtype)

    def step(i, carry):
        for s, relays in RELAY.items():
            @pl.when(i == s)
            def _():
                for relay in relays:
                    for what in ("k", "v"):
                        arrived(what, relay, 0)
                        pass_on(what, relay)
        for what in ("k", "v"):
            arrived(what, i, 1)
        for g in range(num_kv):
            for m in range(2):
                kt = kbuf[i, m, g * head_dim:(g + 1) * head_dim]
                kk[g, m] = jnp.concatenate([kt, kt], axis=0).T
        fill, drain = i // slots, 0
        tops, peaks, alphas, totals, outs, sums = {}, {}, {}, {}, {}, {}

        def scores(h, m):
            keys = kk[h // group, m]
            s = jnp.dot(jnp.concatenate([keys, keys], axis=1), qw[h], preferred_element_type=jnp.float32)
            s_ring[h % (LAG + 1)][fill, m * tokens:(m + 1) * tokens] = s
            top = jnp.max(s.reshape(tokens // 8, 8, tokens), axis=0)
            tops[h] = top if m == 0 else jnp.maximum(tops[h], top)

        def weights(h, m):
            if m == 0:
                m_prev = m_s[h]
                peaks[h] = jnp.maximum(m_prev, jnp.max(tops[h], axis=0, keepdims=True))
                m_s[h] = peaks[h]
                alphas[h] = jnp.exp2(m_prev - peaks[h])
                totals[h] = l_s[h] * alphas[h]
                sums[h] = []
            for r in range(0, tokens, CHUNK):
                peak = peaks[h]
                if len(sums[h]) >= DEPTH:
                    peak = jnp.maximum(peak, jnp.minimum(peak, sums[h][-DEPTH]))
                s = s_ring[h % (LAG + 1)][drain, m * tokens + r:m * tokens + r + CHUNK]
                p = jnp.exp2(s.reshape(CHUNK // 8, 8, tokens) - peak[None])
                totals[h] = totals[h] + jnp.sum(p, axis=0)
                sums[h].append(totals[h])
                p_ring[(2 * h + m) % len(p_ring)][fill, r:r + CHUNK] = p.reshape(CHUNK, tokens).astype(jnp.bfloat16)
            if m == 1:
                l_s[h] = totals[h]

        def values(h, m):
            g = h // group
            out = jnp.dot(vbuf[i, m, g * head_dim:(g + 1) * head_dim], p_ring[(2 * h + m) % len(p_ring)][drain],
                          preferred_element_type=jnp.float32)
            outs[h] = out if m == 0 else outs[h] + out
            if m == 1:
                old = acc[h].reshape(head_dim // 8, 8, tokens) * alphas[h][None]
                acc[h] = old.reshape(head_dim, tokens) + outs[h]

        for u in range(-2 * LAG, 2 * heads + VALUE_LAG):
            for offset, part in ((2 * LAG, scores), (0, weights), (-VALUE_LAG, values)):
                if 0 <= u + offset < 2 * heads:
                    part((u + offset) // 2, (u + offset) % 2)
        return carry

    lax.fori_loop(0, slots, step, 0)
    for h in range(heads):
        total = jnp.sum(l_s[h], axis=0, keepdims=True)
        o_ref[h] = (acc[h] / total).astype(jnp.bfloat16)
    for n, (what, slot) in enumerate(copies):
        buf, _ = bufs[what]
        pltpu.make_async_copy(buf.at[slot, 0], buf.at[slot, 0], send_sem.at[n]).wait()


def solution(mesh):
    size_x = mesh.shape["cx"] // 2
    size_y = mesh.shape["cy"]
    seq_spec = P(("batch", "cx", "cy"), None, None)

    def local_attention(q_local, k_local, v_local):
        tokens, heads, head_dim = q_local.shape
        num_kv = k_local.shape[1]
        q_t = jnp.transpose(q_local, (1, 2, 0))
        k_t = jnp.transpose(k_local, (1, 2, 0)).reshape(num_kv * head_dim, tokens)
        v_t = jnp.transpose(v_local, (1, 2, 0)).reshape(num_kv * head_dim, tokens)
        slots = len(SLOTS)
        f32, bf16 = jnp.float32, jnp.bfloat16
        out = pl.pallas_call(
            functools.partial(attention_kernel, size_x, size_y),
            out_shape=jax.ShapeDtypeStruct((heads, head_dim, tokens), bf16),
            in_specs=[pl.BlockSpec(memory_space=pltpu.HBM)] * 3,
            out_specs=pl.BlockSpec(memory_space=pltpu.VMEM),
            scratch_shapes=[
                pltpu.VMEM((heads, head_dim, tokens), bf16),
                pltpu.VMEM((slots, 2, num_kv * head_dim, tokens), bf16),
                pltpu.VMEM((slots, 2, num_kv * head_dim, tokens), bf16),
                pltpu.VMEM((heads, 256, tokens), bf16),
                pltpu.VMEM((num_kv, 2, tokens, 2 * head_dim), bf16),
                pltpu.VMEM((heads, 8, tokens), f32),
                pltpu.VMEM((heads, 8, tokens), f32),
                pltpu.VMEM((heads, head_dim, tokens), f32),
                pltpu.SemaphoreType.DMA((3,)),
                pltpu.SemaphoreType.DMA((64,)),
                pltpu.SemaphoreType.DMA((slots, 2)),
                pltpu.SemaphoreType.DMA((slots, 2)),
            ] + [pltpu.VMEM((2, 2 * tokens, tokens), f32)] * (LAG + 1) + [pltpu.VMEM((2, tokens, tokens), bf16)] * 4,
            compiler_params=pltpu.CompilerParams(
                collective_id=0, has_side_effects=True, vmem_limit_bytes=20 * 2**20),
            name="attention",
        )(*(pltpu.with_memory_space_constraint(x, pltpu.HBM) for x in (q_t, k_t, v_t)))
        return jnp.transpose(out, (2, 0, 1))

    return jax.shard_map(local_attention, mesh=mesh, in_specs=(seq_spec, seq_spec, seq_spec), out_specs=seq_spec, check_vma=False)
```

```python
import functools
import math
import jax
import jax.numpy as jnp
from jax import lax
from jax.experimental import pallas as pl
from jax.experimental.pallas import tpu as pltpu
from jax.sharding import PartitionSpec as P

SLOTS = [(0, 0), (1, 0), (-1, 0), (0, 1), (0, -1), (1, 1), (1, -1), (-1, 1), (-1, -1), (2, 0), (0, 2),
         (2, 1), (2, -1), (1, 2), (-1, 2), (2, 2)]
SLOT_OF = {offset: slot for slot, offset in enumerate(SLOTS)}
LAG = 3
VALUE_LAG = 2
CHUNK = 128
DEPTH = 3


def wrap(step):
    return (step + 1) % 4 - 1


def send_plan():
    plan = {}

    def add(what, offset, step_x, step_y):
        plan.setdefault((what, SLOT_OF[offset]), []).append((step_x, step_y))

    for what, swap in (("k", False), ("v", True)):
        flip = (lambda pair: (pair[1], pair[0])) if swap else (lambda pair: pair)
        sign = -1 if swap else 1

        def hop(offset, step):
            add(what, flip(offset), *flip(step))

        hop((0, 0), (1, 0))
        hop((0, 0), (-1, 0))
        hop((-sign, 0), (sign, 0))
        for dx in (0, 1, -1, 2):
            hop((dx, 0), (0, 1))
            hop((dx, 0), (0, -1))
            way = sign if dx in (0, 1) else -sign
            hop((dx, -way), (0, way))
    return plan


PLAN = send_plan()
RELAY = {1: (1, 2, 3, 4), 4: (5, 6, 7, 8, 9, 10), 7: (11, 12, 13, 14), 12: (15,)}


def split3(wide):
    hi = wide.astype(jnp.bfloat16)
    rest = wide - hi.astype(jnp.float32)
    mid = rest.astype(jnp.bfloat16)
    low = (rest - mid.astype(jnp.float32)).astype(jnp.bfloat16)
    return hi, mid, low


def attention_kernel(size_x, size_y, q_hbm, k_hbm, v_hbm, o_ref, q_ref, kbuf, vbuf, qw, kk, m_s, l_s, acc, load_sem,
                     send_sem, recv_k, recv_v, *rings):
    heads, head_dim, tokens = q_ref.shape
    num_kv = kbuf.shape[2] // head_dim
    group = heads // num_kv
    slots = len(SLOTS)
    s_ring, p_ring = rings[:LAG + 1], rings[LAG + 1:]
    cx, cy = lax.axis_index("cx"), lax.axis_index("cy")
    core = cx % 2
    chip_x = cx // 2

    def peer(step_x, step_y):
        return {"cx": ((chip_x + step_x + size_x) % size_x) * 2 + core, "cy": (cy + step_y + size_y) % size_y}

    sibling = {"cx": chip_x * 2 + (1 - core), "cy": cy}
    mesh_id = pl.DeviceIdType.MESH

    loads = [pltpu.make_async_copy(src, dst, load_sem.at[n]) for n, (src, dst) in enumerate(
        ((k_hbm, kbuf.at[0, 0]), (v_hbm, vbuf.at[0, 0]), (q_hbm, q_ref)))]
    for load in loads:
        load.start()
    barrier = pltpu.get_barrier_semaphore()
    for device in (peer(1, 0), peer(-1, 0), peer(0, 1), peer(0, -1), sibling):
        pl.semaphore_signal(barrier, inc=1, device_id=device, device_id_type=mesh_id)
    pl.semaphore_wait(barrier, 5)

    bufs = {"k": (kbuf, recv_k), "v": (vbuf, recv_v)}
    copies = []

    def push(what, slot, dst_slot, plane, device):
        buf, recv = bufs[what]
        copies.append((what, slot))
        pltpu.make_async_remote_copy(
            src_ref=buf.at[slot, 0], dst_ref=buf.at[dst_slot, plane], send_sem=send_sem.at[len(copies) - 1],
            recv_sem=recv.at[dst_slot, plane], device_id=device, device_id_type=mesh_id).start()

    def pass_on(what, slot):
        for step_x, step_y in PLAN.get((what, slot), ()):
            dx, dy = SLOTS[slot]
            push(what, slot, SLOT_OF[(wrap(dx - step_x), wrap(dy - step_y))], 0, peer(step_x, step_y))
        push(what, slot, slot, 1, sibling)

    def arrived(what, slot, plane):
        buf, recv = bufs[what]
        pltpu.make_async_copy(buf.at[slot, plane], buf.at[slot, plane], recv.at[slot, plane]).wait()

    for what, load in zip(("k", "v"), loads):
        load.wait()
        pass_on(what, 0)
    loads[2].wait()

    scale = math.log2(math.e) / math.sqrt(head_dim)
    for h in range(heads):
        hi, mid, low = split3(q_ref[h].astype(jnp.float32) * scale)
        qw[h, 0:head_dim] = hi
        qw[h, head_dim:2 * head_dim] = mid
        qw[h, 2 * head_dim:3 * head_dim] = low
        qw[h, 3 * head_dim:] = jnp.zeros_like(hi)
    m_s[...] = jnp.full(m_s.shape, -jnp.inf, jnp.float32)
    for ref in (l_s, acc):
        ref[...] = jnp.zeros(ref.shape, ref.dtype)

    def step(i, carry):
        for s, relays in RELAY.items():
            @pl.when(i == s)
            def _():
                for relay in relays:
                    for what in ("k", "v"):
                        arrived(what, relay, 0)
                        pass_on(what, relay)
        for what in ("k", "v"):
            arrived(what, i, 1)
        for g in range(num_kv):
            for m in range(2):
                kt = kbuf[i, m, g * head_dim:(g + 1) * head_dim]
                kk[g, m] = jnp.concatenate([kt, kt], axis=0).T
        fill, drain = i // slots, 0
        tops, peaks, alphas, totals, outs, sums = {}, {}, {}, {}, {}, {}

        def scores(h, m):
            keys = kk[h // group, m]
            s = jnp.dot(jnp.concatenate([keys, keys], axis=1), qw[h], preferred_element_type=jnp.float32)
            s_ring[h % (LAG + 1)][fill, m * tokens:(m + 1) * tokens] = s
            top = jnp.max(s.reshape(tokens // 8, 8, tokens), axis=0)
            tops[h] = top if m == 0 else jnp.maximum(tops[h], top)

        def weights(h, m):
            if m == 0:
                m_prev = m_s[h]
                peaks[h] = jnp.maximum(m_prev, jnp.max(tops[h], axis=0, keepdims=True))
                m_s[h] = peaks[h]
                alphas[h] = jnp.exp2(m_prev - peaks[h])
                totals[h] = l_s[h] * alphas[h]
                sums[h] = []
            for r in range(0, tokens, CHUNK):
                peak = peaks[h]
                if len(sums[h]) >= DEPTH:
                    peak = jnp.maximum(peak, jnp.minimum(peak, sums[h][-DEPTH]))
                s = s_ring[h % (LAG + 1)][drain, m * tokens + r:m * tokens + r + CHUNK]
                p = jnp.exp2(s.reshape(CHUNK // 8, 8, tokens) - peak[None])
                totals[h] = totals[h] + jnp.sum(p, axis=0)
                sums[h].append(totals[h])
                p_ring[(2 * h + m) % len(p_ring)][fill, r:r + CHUNK] = p.reshape(CHUNK, tokens).astype(jnp.bfloat16)
            if m == 1:
                l_s[h] = totals[h]

        def values(h, m):
            g = h // group
            out = jnp.dot(vbuf[i, m, g * head_dim:(g + 1) * head_dim], p_ring[(2 * h + m) % len(p_ring)][drain],
                          preferred_element_type=jnp.float32)
            outs[h] = out if m == 0 else outs[h] + out
            if m == 1:
                old = acc[h].reshape(head_dim // 8, 8, tokens) * alphas[h][None]
                acc[h] = old.reshape(head_dim, tokens) + outs[h]

        for u in range(-2 * LAG, 2 * heads + VALUE_LAG):
            for offset, part in ((2 * LAG, scores), (0, weights), (-VALUE_LAG, values)):
                if 0 <= u + offset < 2 * heads:
                    part((u + offset) // 2, (u + offset) % 2)
        return carry

    lax.fori_loop(0, slots, step, 0)
    for h in range(heads):
        total = jnp.sum(l_s[h], axis=0, keepdims=True)
        o_ref[h] = (acc[h] / total).astype(jnp.bfloat16)
    for n, (what, slot) in enumerate(copies):
        buf, _ = bufs[what]
        pltpu.make_async_copy(buf.at[slot, 0], buf.at[slot, 0], send_sem.at[n]).wait()


def solution(mesh):
    size_x = mesh.shape["cx"] // 2
    size_y = mesh.shape["cy"]
    seq_spec = P(("batch", "cx", "cy"), None, None)

    def local_attention(q_local, k_local, v_local):
        tokens, heads, head_dim = q_local.shape
        num_kv = k_local.shape[1]
        q_t = jnp.transpose(q_local, (1, 2, 0))
        k_t = jnp.transpose(k_local, (1, 2, 0)).reshape(num_kv * head_dim, tokens)
        v_t = jnp.transpose(v_local, (1, 2, 0)).reshape(num_kv * head_dim, tokens)
        slots = len(SLOTS)
        f32, bf16 = jnp.float32, jnp.bfloat16
        out = pl.pallas_call(
            functools.partial(attention_kernel, size_x, size_y),
            out_shape=jax.ShapeDtypeStruct((heads, head_dim, tokens), bf16),
            in_specs=[pl.BlockSpec(memory_space=pltpu.HBM)] * 3,
            out_specs=pl.BlockSpec(memory_space=pltpu.VMEM),
            scratch_shapes=[
                pltpu.VMEM((heads, head_dim, tokens), bf16),
                pltpu.VMEM((slots, 2, num_kv * head_dim, tokens), bf16),
                pltpu.VMEM((slots, 2, num_kv * head_dim, tokens), bf16),
                pltpu.VMEM((heads, 256, tokens), bf16),
                pltpu.VMEM((num_kv, 2, tokens, 2 * head_dim), bf16),
                pltpu.VMEM((heads, 8, tokens), f32),
                pltpu.VMEM((heads, 8, tokens), f32),
                pltpu.VMEM((heads, head_dim, tokens), f32),
                pltpu.SemaphoreType.DMA((3,)),
                pltpu.SemaphoreType.DMA((64,)),
                pltpu.SemaphoreType.DMA((slots, 2)),
                pltpu.SemaphoreType.DMA((slots, 2)),
            ] + [pltpu.VMEM((2, 2 * tokens, tokens), f32)] * (LAG + 1) + [pltpu.VMEM((2, tokens, tokens), bf16)] * 4,
            compiler_params=pltpu.CompilerParams(
                collective_id=0, has_side_effects=True, vmem_limit_bytes=20 * 2**20),
            name="attention",
        )(*(pltpu.with_memory_space_constraint(x, pltpu.HBM) for x in (q_t, k_t, v_t)))
        return jnp.transpose(out, (2, 0, 1))

    return jax.shard_map(local_attention, mesh=mesh, in_specs=(seq_spec, seq_spec, seq_spec), out_specs=seq_spec, check_vma=False)
```
